32 devices in a mesh: ep: 8 (over z, x), etp: 4 (over y, core).
Axes of the slice: x: 2, y: 2, z: 4, core: 2. Of those that a mesh axis runs over, the one named last changes fastest.
Arguments:
- tokens: bfloat16 [1024, 4096], P('ep', 'etp'), may hold values from -6 to 6
- expert_ids: int32 [1024, 8], P('ep'), may hold values from 0 to 15, all different within a row; in each aligned block of 128 rows (0 to 127, 128 to 255, ...) at most 96 rows name the same one
- gate_prob: float32 [1024, 8], P('ep'), may hold values from 0.05 to 1
- gate_weight: bfloat16 [16, 4096, 1536], P('ep', None, 'etp'), may hold values from -0.09375 to 0.09375
- up_weight: bfloat16 [16, 4096, 1536], P('ep', None, 'etp'), may hold values from -0.09375 to 0.09375
- down_weight: bfloat16 [16, 1536, 4096], P('ep', 'etp'), may hold values from -0.15625 to 0.15625
Outputs:
- mixed: bfloat16 [1024, 4096], P('ep', 'etp')
The draws below stay inside these ranges and needn't reach their ends.
Inputs may be any that keep to these rules, and one draw needn't show every extreme that they name: `expert_ids`: each row names 8 different experts. Within each aligned block of 128 rows (one token group) no expert is named more than 96 times, and in every draw some expert is named exactly 96 times in some block.
All inputs are finite; a program needn't handle non-finite values.
Results may differ from the reference program's by a relative error of at most 0.012.
Values may be sent and summed in bfloat16 or wider, within the bound.
A program may use at most 128 MiB of HBM per device.

```python
import math
import jax
import jax.numpy as jnp
import numpy as np
from jax import lax

D = 4096
FF = 1536
TOP = 8
TOK_DEV = 128
EXPERTS = 16
GROUPS = 8
TOKENS = 1024
CAP = 96
N_ETP = 4


def shard_levels(rng, shape, split, least, top_value):
    level, own = 1.0, jax.random.fold_in(rng, 6)
    for dim, shards_of in split:
        draws = jnp.exp(jax.random.uniform(jax.random.fold_in(own, dim), (shards_of,), jnp.float32, least / len(split), top_value / len(split)))
        level = level * jnp.repeat(draws, shape[dim] // shards_of).reshape([-1 if axis == dim else 1 for axis in range(len(shape))])
    return level


def assign_block(stream_key, own, number, rows, count, top, most, lean):
    ranking = jax.random.permutation(stream_key, count)
    packed, ordinary = load_shares(count, rows * top, most, lean, True), load_shares(count, rows * top, most, lean, False)
    places = jnp.arange(count)

    def named(lengths, offset_by):
        used = int((lengths > 0).sum())
        fixed = max(1, used // 4)
        moved = fixed + (places - fixed + offset_by * (used - fixed)) % max(1, count - fixed)
        return jnp.zeros((count,), jnp.int32).at[ranking[jnp.where(places < fixed, places, moved)]].set(jnp.asarray(lengths, jnp.int32))

    lengths = jnp.where(number % 4 == 0, named(packed, number // 4), named(ordinary, number - number // 4 - 1))
    mixed = jax.random.permutation(jax.random.fold_in(own, 3), count)
    source_of, sink = mixed[0:count // 2 * 2:2], mixed[1:count // 2 * 2:2]
    slack = jnp.minimum(lengths[source_of] - 1, most - lengths[sink]) // 2
    slack = jnp.where((source_of == ranking[0]) | (sink == ranking[0]) | (lengths[sink] == 0), 0, jnp.maximum(slack, 0))
    moved = jax.random.randint(jax.random.fold_in(own, 4), (count // 2,), 0, 1 << 20) % (slack + 1)
    lengths = lengths.at[source_of].add(-moved).at[sink].add(moved)
    items = jnp.searchsorted(jnp.cumsum(lengths), jnp.arange(rows * top), side="right").astype(jnp.int32)
    grid = items.reshape(top, rows).T
    grid = grid[jax.random.permutation(jax.random.fold_in(own, 1), rows)]
    offset_by = jax.random.randint(jax.random.fold_in(own, 2), (rows, 1), 0, top)
    return jnp.take_along_axis(grid, (jnp.arange(top)[None, :] + offset_by) % top, axis=1)


def load_shares(amount, total, limit, slope, full):
    weights = [(1 << 20) // math.isqrt(standing ** slope) + 1 for standing in range(1, amount + 1)]
    largest = limit if full else min(limit, max(-(-total // amount), total * weights[0] // sum(weights)))
    least = 1 if total - largest >= amount - 1 else 0
    given, rest = [largest] + [least] * (amount - 1), total - largest - least * (amount - 1)
    while rest > 0:
        free = [i for i in range(1, amount) if given[i] < largest] or [i for i in range(1, amount) if given[i] < limit]
        whole, remaining = sum([weights[i] for i in free]), rest
        for i in free:
            more = min(limit - given[i], max(1, remaining * weights[i] // whole), rest)
            given[i] = given[i] + more
            rest = rest - more
    return np.array(given)


def scatter_about(own_key, dims, spread, most, pieces=(), kind=jnp.bfloat16):
    result = jax.random.normal(own_key, dims, jnp.float32) * spread
    if len(pieces) > 0:
        result = shard_levels(own_key, dims, pieces, -0.22, 0.18) * result
    return jnp.clip(result, min=-most, max=most).astype(kind)


def setup_inputs(seed: int = 0) -> dict:
    splits = jax.random.split(jax.random.key(seed), 7)
    tokens = scatter_about(splits[0], (TOKENS, D), 1.0, 6.0, ((0, 8), (1, 4)))
    expert_ids_keys = jax.random.split(jax.random.fold_in(splits[1], 1), TOKENS // TOK_DEV)
    expert_ids_turns = jax.random.permutation(jax.random.fold_in(splits[1], 3), TOKENS // TOK_DEV)
    expert_ids = jax.vmap(lambda own, number: assign_block(jax.random.fold_in(splits[1], 2), own, number, TOK_DEV, EXPERTS, TOP, CAP, 2))(expert_ids_keys, expert_ids_turns).reshape((TOKENS, TOP))
    gate_prob = jnp.clip(0.05 + 0.95 * jax.random.uniform(splits[2], (TOKENS, TOP), jnp.float32) ** shard_levels(splits[2], (TOKENS, TOP), ((0, 8),), -0.2, 0.2), 0.05, 1.0)
    gate_weight = scatter_about(splits[3], (EXPERTS, D, FF), D ** -0.5, 0.09375, ((0, 8), (2, 4)))
    up_weight = scatter_about(splits[4], (EXPERTS, D, FF), D ** -0.5, 0.09375, ((0, 8), (2, 4)))
    down_weight = scatter_about(splits[5], (EXPERTS, FF, D), FF ** -0.5, 0.15625, ((0, 8), (1, 4)))
    return dict(tokens=tokens, expert_ids=expert_ids, gate_prob=gate_prob, gate_weight=gate_weight, up_weight=up_weight, down_weight=down_weight)


def reference(tokens, expert_ids, gate_prob, gate_weight, up_weight, down_weight):
    assigned = TOK_DEV * TOP
    grouped = expert_ids.reshape(GROUPS, assigned).astype(jnp.int32)
    onehot = (grouped[:, :, None] == jnp.arange(EXPERTS, dtype=jnp.int32)[None, None, :]).astype(jnp.int32)
    position = jnp.sum((jnp.cumsum(onehot, axis=1) - onehot) * onehot, axis=2).astype(jnp.int32)
    slot_index = (grouped * CAP + position).astype(jnp.int32)
    group_rows = jnp.arange(GROUPS, dtype=jnp.int32)[:, None]
    owners = (group_rows * TOK_DEV + (jnp.arange(assigned, dtype=jnp.int32) // TOP)[None, :]).astype(jnp.int32)
    sources = jnp.full((GROUPS, EXPERTS * CAP), TOKENS, jnp.int32).at[group_rows, slot_index].set(owners)
    scales = jnp.zeros((GROUPS, EXPERTS * CAP), jnp.float32).at[group_rows, slot_index].set(
        gate_prob.reshape(GROUPS, assigned).astype(jnp.float32))
    sources = sources.reshape(GROUPS, EXPERTS, CAP).transpose(1, 0, 2).reshape(EXPERTS, GROUPS * CAP)
    scales = scales.reshape(GROUPS, EXPERTS, CAP).transpose(1, 0, 2).reshape(EXPERTS, GROUPS * CAP)
    padded = jnp.concatenate([tokens, jnp.zeros((1, D), tokens.dtype)], axis=0)
    block = FF // N_ETP

    def expert_step(accumulated, inputs):
        w_gate, w_up, w_down, rows_from, row_scale = inputs
        expert_rows = padded[rows_from]
        gate_sum = jnp.dot(expert_rows, w_gate, preferred_element_type=jnp.float32)
        up_sum = jnp.dot(expert_rows, w_up, preferred_element_type=jnp.float32)
        hidden = (jax.nn.silu(gate_sum) * up_sum).astype(jnp.bfloat16)
        expert_out = jnp.zeros((GROUPS * CAP, D), jnp.float32)
        for part_index in range(N_ETP):
            product = jnp.dot(hidden[:, part_index * block:(part_index + 1) * block],
                              w_down[part_index * block:(part_index + 1) * block, :],
                              preferred_element_type=jnp.float32)
            rounded = lax.optimization_barrier(product.astype(jnp.bfloat16))
            expert_out = expert_out + rounded.astype(jnp.float32)
        accumulated = accumulated.at[rows_from].add(row_scale[:, None] * expert_out)
        return accumulated, None

    accumulated = jnp.zeros((TOKENS + 1, D), jnp.float32)
    accumulated, unused = lax.scan(expert_step, accumulated,
                                   (gate_weight, up_weight, down_weight, sources, scales))
    return accumulated[:TOKENS].astype(jnp.bfloat16)
```

```python
import functools

import jax
import jax.numpy as jnp
from jax import lax
from jax.experimental import pallas as pl
from jax.experimental.pallas import tpu as pltpu
from jax.sharding import PartitionSpec as P

MESH = pl.DeviceIdType.MESH
VMEM_BUDGET = 16 << 20


def place(sizes):
    ep, etp = lax.axis_index("ep"), lax.axis_index("etp")
    return (ep // 2, ep % 2, etp // 2, etp % 2)


def moved(here, sizes, rel):
    return tuple((h + r) % n if r else h for h, n, r in zip(here, sizes, rel))


def device(at):
    z, x, y, c = at
    return (z * 2 + x, y * 2 + c)


def barrier(here, sizes, rels):
    sem = pltpu.get_barrier_semaphore()
    for rel in rels:
        pl.semaphore_signal(sem, inc=1, device_id=device(moved(here, sizes, rel)), device_id_type=MESH)
    pl.semaphore_wait(sem, len(rels))


def gather_kernel(sizes, x_ref, w_ref, out_ref, w_out_ref, send_sem, recv_sem, w_send, w_recv, own_sem):
    nz = sizes[0]
    rows, cols = x_ref.shape
    half = rows // 2
    here = place(sizes)
    z_rels = [(d, 0, 0, 0) for d in range(1, nz)]
    ep_rels = [(d, e, 0, 0) for d in range(nz) for e in range(2) if d or e]
    barrier(here, sizes, ep_rels + [(0, 0, 1, 0), (0, 0, 0, 1)])

    def number(rel):
        return ((rel[0] * 2 + rel[1]) * 2 + rel[2]) * 2 + rel[3]

    def slot(h, rel):
        group, member = device(moved(here, sizes, rel))
        return out_ref.at[pl.ds(pl.multiple_of(group * rows + h * half, half), half),
                          pl.ds(pl.multiple_of(member * cols, cols), cols)]

    sends = []

    def send(h, rel, step):
        lands = tuple((r - s) % n for r, s, n in zip(rel, step, sizes))
        src = slot(h, rel) if any(rel) else x_ref.at[pl.ds(h * half, half), :]
        copy = pltpu.make_async_remote_copy(
            src_ref=src, dst_ref=slot(h, rel), send_sem=send_sem.at[len(sends)],
            recv_sem=recv_sem.at[h, number(lands)],
            device_id=device(moved(here, sizes, step)), device_id_type=MESH)
        copy.start()
        sends.append(copy)

    def arrive(h, rel):
        ref = slot(h, rel)
        pltpu.make_async_copy(ref, ref, recv_sem.at[h, number(rel)]).wait()

    first = {0: (0, 1, 0, 0), 1: (0, 0, 1, 0)}
    second = {0: (0, 0, 1, 0), 1: (0, 1, 0, 0)}
    other = (0, 0, 0, 1)

    own = pltpu.make_async_copy(
        x_ref, out_ref.at[pl.ds(pl.multiple_of(device(here)[0] * rows, rows), rows),
                          pl.ds(pl.multiple_of(device(here)[1] * cols, cols), cols)], own_sem)
    own.start()
    for step in z_rels:
        for h in range(2):
            send(h, (0, 0, 0, 0), step)
    for h in range(2):
        send(h, (0, 0, 0, 0), first[h])
    for h in range(2):
        send(h, (0, 0, 0, 0), second[h])
    for h in range(2):
        send(h, (0, 0, 0, 0), other)
    w_sends = []
    me = device(here)[0]
    for i, rel in enumerate(ep_rels):
        back = tuple((-r) % n for r, n in zip(rel, sizes))
        copy = pltpu.make_async_remote_copy(
            src_ref=w_ref, dst_ref=w_out_ref.at[me], send_sem=w_send.at[i],
            recv_sem=w_recv.at[ep_rels.index(back)],
            device_id=device(moved(here, sizes, rel)), device_id_type=MESH)
        copy.start()
        w_sends.append(copy)
    w_own = pltpu.make_async_copy(w_ref, w_out_ref.at[me], w_recv.at[len(ep_rels)])
    w_own.start()
    order = sorted(range(1, nz), key=lambda d: min(d, nz - d))
    for d in order:
        for h in range(2):
            arrive(h, (d, 0, 0, 0))
            send(h, (d, 0, 0, 0), first[h])
            send(h, (d, 0, 0, 0), second[h])
            send(h, (d, 0, 0, 0), other)
    for d in [0] + order:
        for h in range(2):
            rel = (d,) + first[h][1:]
            arrive(h, rel)
            send(h, rel, second[h])
            send(h, rel, other)
    for d in [0] + order:
        for h in range(2):
            rel = (d,) + second[h][1:]
            arrive(h, rel)
            send(h, rel, other)
    for d in [0] + order:
        for h in range(2):
            rel = (d, 1, 1, 0)
            arrive(h, rel)
            send(h, rel, other)
    for d in range(nz):
        for e in range(2):
            for f in range(2):
                for h in range(2):
                    arrive(h, (d, e, f, 1))
    for i in range(len(ep_rels)):
        w_sends[i].wait_send()
        ref = w_out_ref.at[0]
        pltpu.make_async_copy(ref, ref, w_recv.at[i]).wait()
    for copy in sends:
        copy.wait_send()
    own.wait()
    w_own.wait()


def gather(sizes, x, w):
    groups, parts = sizes[0] * sizes[1], sizes[2] * sizes[3]
    rows, cols = x.shape
    n_send = 2 * (sizes[0] - 1 + sizes[0] + 2 * sizes[0] + 4 * sizes[0])
    return pl.pallas_call(
        functools.partial(gather_kernel, sizes),
        out_shape=(jax.ShapeDtypeStruct((groups * rows, parts * cols), x.dtype),
                   jax.ShapeDtypeStruct((groups,) + w.shape, w.dtype)),
        in_specs=[pl.BlockSpec(memory_space=pltpu.VMEM)] * 2,
        out_specs=(pl.BlockSpec(memory_space=pl.ANY), pl.BlockSpec(memory_space=pltpu.VMEM)),
        scratch_shapes=[
            pltpu.SemaphoreType.DMA((n_send,)),
            pltpu.SemaphoreType.DMA((2, groups * parts)),
            pltpu.SemaphoreType.DMA((groups - 1,)),
            pltpu.SemaphoreType.DMA((groups,)),
            pltpu.SemaphoreType.DMA,
        ],
        compiler_params=pltpu.CompilerParams(collective_id=0, has_side_effects=True, vmem_limit_bytes=16 << 20),
        name="gather_tokens",
    )(x, w)


def scatter_kernel(sizes, p_ref, out_ref, buf_c, buf_1, buf_2, buf_z, send_sem, recv_c, recv_1, recv_2, recv_z):
    nz = sizes[0]
    rows, cols = out_ref.shape
    half = rows // 2
    here = place(sizes)
    barrier(here, sizes, [(d, 0, 0, 0) for d in range(1, nz)] + [(0, 1, 0, 0), (0, 0, 1, 0), (0, 0, 0, 1)])
    axis = ((0, 1, 0, 0), (0, 0, 1, 0))
    first = {0: axis[1], 1: axis[0]}
    second = {0: axis[0], 1: axis[1]}
    sends = []

    def local(h, rel):
        group, member = device(moved(here, sizes, rel))
        return p_ref.at[pl.ds(pl.multiple_of(group * rows + h * half, half), half),
                        pl.ds(pl.multiple_of(member * cols, cols), cols)]

    def rel_of(h, a, b, d):
        e, f = (b, a) if h == 0 else (a, b)
        return (d, e, f)

    def send(src, dst, recv, step):
        copy = pltpu.make_async_remote_copy(
            src_ref=src, dst_ref=dst, send_sem=send_sem.at[len(sends)], recv_sem=recv,
            device_id=device(moved(here, sizes, step)), device_id_type=MESH)
        copy.start()
        sends.append(copy)

    def arrive(ref, sem):
        pltpu.make_async_copy(ref, ref, sem).wait()

    def add(dst, *srcs):
        chunk = 16

        @pl.loop(0, half // chunk)
        def _(i):
            at = pl.ds(pl.multiple_of(i * chunk, chunk), chunk)
            total = srcs[0][at, :].astype(jnp.float32)
            for src in srcs[1:]:
                total = total + src[at, :].astype(jnp.float32)
            dst[at, :] = total.astype(dst.dtype)

    zs = list(range(1, nz)) + [0]
    for a, b in ((1, 1), (1, 0), (0, 1), (0, 0)):
        for d in zs:
            for h in range(2):
                send(local(h, rel_of(h, a, b, d) + (1,)), buf_c.at[h, a, b, d], recv_c.at[h, a, b, d], (0, 0, 0, 1))
    for b in (1, 0):
        for d in zs:
            for h in range(2):
                piece = buf_c.at[h, 1, b, d]
                arrive(piece, recv_c.at[h, 1, b, d])
                add(piece, piece, local(h, rel_of(h, 1, b, d) + (0,)))
                send(piece, buf_1.at[h, b, d], recv_1.at[h, b, d], first[h])
    for d in zs:
        for h in range(2):
            piece = buf_c.at[h, 0, 1, d]
            arrive(piece, recv_c.at[h, 0, 1, d])
            arrive(buf_1.at[h, 1, d], recv_1.at[h, 1, d])
            add(piece, piece, local(h, rel_of(h, 0, 1, d) + (0,)), buf_1.at[h, 1, d])
            send(piece, buf_2.at[h, d], recv_2.at[h, d], second[h])
    for d in zs:
        for h in range(2):
            piece = buf_c.at[h, 0, 0, d]
            arrive(piece, recv_c.at[h, 0, 0, d])
            arrive(buf_1.at[h, 0, d], recv_1.at[h, 0, d])
            arrive(buf_2.at[h, d], recv_2.at[h, d])
            srcs = (piece, local(h, rel_of(h, 0, 0, d) + (0,)), buf_1.at[h, 0, d], buf_2.at[h, d])
            if d:
                add(piece, *srcs)
                send(piece, buf_z.at[h, nz - d - 1], recv_z.at[h, nz - d - 1], (d, 0, 0, 0))
            else:
                for k in range(nz - 1):
                    arrive(buf_z.at[h, k], recv_z.at[h, k])
                add(out_ref.at[pl.ds(h * half, half), :], *srcs, *[buf_z.at[h, k] for k in range(nz - 1)])
    for copy in sends:
        copy.wait_send()


def scatter(sizes, p):
    nz = sizes[0]
    groups, parts = nz * 2, sizes[2] * sizes[3]
    rows, cols = p.shape[0] // groups, p.shape[1] // parts
    half = rows // 2
    n_send = 2 * (4 * nz + 2 * nz + nz + nz - 1)
    return pl.pallas_call(
        functools.partial(scatter_kernel, sizes),
        out_shape=jax.ShapeDtypeStruct((rows, cols), p.dtype),
        in_specs=[pl.BlockSpec(memory_space=pltpu.VMEM)],
        out_specs=pl.BlockSpec(memory_space=pltpu.VMEM),
        scratch_shapes=[
            pltpu.VMEM((2, 2, 2, nz, half, cols), p.dtype),
            pltpu.VMEM((2, 2, nz, half, cols), p.dtype),
            pltpu.VMEM((2, nz, half, cols), p.dtype),
            pltpu.VMEM((2, nz - 1, half, cols), p.dtype),
            pltpu.SemaphoreType.DMA((n_send,)),
            pltpu.SemaphoreType.DMA((2, 2, 2, nz)),
            pltpu.SemaphoreType.DMA((2, 2, nz)),
            pltpu.SemaphoreType.DMA((2, nz)),
            pltpu.SemaphoreType.DMA((2, nz - 1)),
        ],
        compiler_params=pltpu.CompilerParams(collective_id=1, has_side_effects=True, vmem_limit_bytes=40 << 20),
        name="reduce_scatter",
    )(p)


def hidden_kernel(x_ref, w_ref, gate_ref, up_ref, out_ref):
    gate = jnp.dot(x_ref[...], gate_ref[0], preferred_element_type=jnp.float32)
    up = jnp.dot(x_ref[...], up_ref[0], preferred_element_type=jnp.float32)
    out_ref[...] = (jax.nn.silu(gate) * up * w_ref[0]).astype(out_ref.dtype)


def down_kernel(h_ref, down_ref, out_ref):
    out_ref[...] = jnp.dot(h_ref[...], down_ref[...], preferred_element_type=jnp.float32).astype(out_ref.dtype)


def tile_of(total, wanted):
    while total % wanted:
        wanted //= 2
    return wanted


def experts_dense(x, scale, gate_weight, up_weight, down_weight):
    members, width, units = gate_weight.shape
    rows = x.shape[0]
    tile = tile_of(rows, 256)
    hidden = pl.pallas_call(
        hidden_kernel,
        grid=(members, rows // tile),
        out_shape=jax.ShapeDtypeStruct((rows, members * units), x.dtype),
        in_specs=[
            pl.BlockSpec((tile, width), lambda e, m: (m, 0)),
            pl.BlockSpec((1, tile, 1), lambda e, m: (e, m, 0)),
            pl.BlockSpec((1, width, units), lambda e, m: (e, 0, 0)),
            pl.BlockSpec((1, width, units), lambda e, m: (e, 0, 0)),
        ],
        out_specs=pl.BlockSpec((tile, units), lambda e, m: (m, e)),
        compiler_params=pltpu.CompilerParams(vmem_limit_bytes=40 << 20),
        name="hidden",
    )(x, scale, gate_weight, up_weight)
    down = down_weight.reshape(members * units, width)
    tile_n = tile_of(width, 512)
    tile_m = tile_of(rows, 1024)
    return pl.pallas_call(
        down_kernel,
        grid=(rows // tile_m, width // tile_n),
        out_shape=jax.ShapeDtypeStruct((rows, width), x.dtype),
        in_specs=[
            pl.BlockSpec((tile_m, members * units), lambda m, n: (m, 0)),
            pl.BlockSpec((members * units, tile_n), lambda m, n: (0, n)),
        ],
        out_specs=pl.BlockSpec((tile_m, tile_n), lambda m, n: (m, n)),
        compiler_params=pltpu.CompilerParams(vmem_limit_bytes=24 << 20),
        name="down",
    )(hidden, down)


def body(tokens, expert_ids, gate_prob, gate_weight, up_weight, down_weight):
    groups, parts = lax.axis_size("ep"), lax.axis_size("etp")
    members = gate_weight.shape[0]
    numbers = jnp.arange(members * groups, dtype=jnp.int32)
    share = jnp.sum(jnp.where(numbers[:, None, None] == expert_ids[None], gate_prob[None], 0.0), axis=2)
    size = groups * parts * tokens.size * tokens.dtype.itemsize
    kernels = groups % 2 == 0 and groups > 2 and parts == 4 and size <= VMEM_BUDGET
    sizes = (groups // 2, 2, parts // 2, 2)
    if kernels:
        gathered, shares = gather(sizes, tokens, share)
    else:
        gathered = lax.all_gather(lax.all_gather(tokens, "ep", axis=0, tiled=True), "etp", axis=1, tiled=True)
        shares = lax.all_gather(share, "ep", axis=0)
    mine = lax.dynamic_slice_in_dim(shares, lax.axis_index("ep") * members, members, axis=1)
    scale = jnp.transpose(mine, (1, 0, 2)).reshape(members, -1, 1)
    partial_sum = experts_dense(gathered, scale, gate_weight, up_weight, down_weight)
    if kernels:
        return scatter(sizes, partial_sum)
    summed = lax.psum_scatter(partial_sum, "etp", scatter_dimension=1, tiled=True)
    return lax.psum_scatter(summed, "ep", scatter_dimension=0, tiled=True)


def solution(mesh):
    in_specs = (
        P("ep", "etp"),
        P("ep", None),
        P("ep", None),
        P("ep", None, "etp"),
        P("ep", None, "etp"),
        P("ep", "etp", None),
    )
    out_specs = P("ep", "etp")
    return jax.shard_map(body, mesh=mesh, in_specs=in_specs, out_specs=out_specs, check_vma=False)
```

```python
import functools

import jax
import jax.numpy as jnp
from jax import lax
from jax.experimental import pallas as pl
from jax.experimental.pallas import tpu as pltpu
from jax.sharding import PartitionSpec as P

MESH = pl.DeviceIdType.MESH
VMEM_BUDGET = 16 << 20


def place(sizes):
    ep, etp = lax.axis_index("ep"), lax.axis_index("etp")
    return (ep // 2, ep % 2, etp // 2, etp % 2)


def flip(at, bits):
    bit = 1
    while bit <= bits:
        if bits & bit:
            at = at + bit - 2 * bit * ((at // bit) % 2)
        bit *= 2
    return at


def moved(here, sizes, rel):
    return tuple(flip(h, r) for h, r in zip(here, rel))


def device(at):
    z, x, y, c = at
    return (z * 2 + x, y * 2 + c)


def barrier(here, sizes, rels):
    sem = pltpu.get_barrier_semaphore()
    for rel in rels:
        pl.semaphore_signal(sem, inc=1, device_id=device(moved(here, sizes, rel)), device_id_type=MESH)
    pl.semaphore_wait(sem, len(rels))


def gather_kernel(sizes, x_ref, w_ref, gate_hbm, up_hbm, hidden_ref, out_ref, w_out_ref,
                  gate_ref, up_ref, send_sem, recv_sem, w_send, w_recv, own_sem, load_sem):
    nz = sizes[0]
    rows, cols = x_ref.shape
    half = rows // 2
    here = place(sizes)
    z_rels = [(d, 0, 0, 0) for d in range(1, nz)]
    ep_rels = [(d, e, 0, 0) for d in range(nz) for e in range(2) if d or e]
    barrier(here, sizes, ep_rels + [(0, 0, 1, 0), (0, 0, 0, 1)])

    def number(rel):
        return ((rel[0] * 2 + rel[1]) * 2 + rel[2]) * 2 + rel[3]

    def slot(h, rel):
        group, member = device(moved(here, sizes, rel))
        return out_ref.at[pl.ds(pl.multiple_of(group * rows + h * half, half), half),
                          pl.ds(pl.multiple_of(member * cols, cols), cols)]

    sends = []

    def send(h, rel, step):
        lands = tuple(r ^ s for r, s in zip(rel, step))
        src = slot(h, rel) if any(rel) else x_ref.at[pl.ds(h * half, half), :]
        copy = pltpu.make_async_remote_copy(
            src_ref=src, dst_ref=slot(h, rel), send_sem=send_sem.at[len(sends)],
            recv_sem=recv_sem.at[h, number(lands)],
            device_id=device(moved(here, sizes, step)), device_id_type=MESH)
        copy.start()
        sends.append(copy)

    def arrive(h, rel):
        ref = slot(h, rel)
        pltpu.make_async_copy(ref, ref, recv_sem.at[h, number(rel)]).wait()

    first = {0: (0, 1, 0, 0), 1: (0, 0, 1, 0)}
    second = {0: (0, 0, 1, 0), 1: (0, 1, 0, 0)}
    other = (0, 0, 0, 1)

    def pass_on(d):
        for h in range(2):
            if d:
                arrive(h, (d, 0, 0, 0))
            send(h, (d, 0, 0, 0), first[h])
            send(h, (d, 0, 0, 0), second[h])
            send(h, (d, 0, 0, 0), other)

    def pass_second(d):
        for h in range(2):
            rel = (d,) + first[h][1:]
            arrive(h, rel)
            send(h, rel, second[h])
            send(h, rel, other)

    def pass_last(d):
        for h in range(2):
            for rel in ((d,) + second[h][1:], (d, 1, 1, 0)):
                arrive(h, rel)
                send(h, rel, other)

    own = pltpu.make_async_copy(
        x_ref, out_ref.at[pl.ds(pl.multiple_of(device(here)[0] * rows, rows), rows),
                          pl.ds(pl.multiple_of(device(here)[1] * cols, cols), cols)], own_sem)
    own.start()
    for step in z_rels[:1]:
        for h in range(2):
            send(h, (0, 0, 0, 0), step)
    pass_on(0)
    for step in z_rels[1:]:
        for h in range(2):
            send(h, (0, 0, 0, 0), step)
    w_sends = []
    me = device(here)[0]
    for i, rel in enumerate(ep_rels):
        copy = pltpu.make_async_remote_copy(
            src_ref=w_ref, dst_ref=w_out_ref.at[me], send_sem=w_send.at[i],
            recv_sem=w_recv.at[i],
            device_id=device(moved(here, sizes, rel)), device_id_type=MESH)
        copy.start()
        w_sends.append(copy)
    w_own = pltpu.make_async_copy(w_ref, w_out_ref.at[me], w_recv.at[len(ep_rels)])
    w_own.start()
    loads = [pltpu.make_async_copy(gate_hbm, gate_ref, load_sem.at[0]),
             pltpu.make_async_copy(up_hbm, up_ref, load_sem.at[1])]
    for load in loads:
        load.start()
    members, units = gate_ref.shape[0], gate_ref.shape[2]

    def compute(d):
        for e in range(2):
            for f in range(2):
                for h in range(2):
                    arrive(h, (d, e, f, 1))
        first_group = flip(here[0], d) * 2
        at = pl.ds(pl.multiple_of(first_group * rows, 2 * rows), 2 * rows)
        x = out_ref[at, :]
        share = w_out_ref[pl.ds(first_group, 2)].reshape(2 * rows, w_ref.shape[1])
        lane = lax.broadcasted_iota(jnp.int32, share.shape, 1)
        for m in range(members):
            scale = jnp.sum(jnp.where(lane == me * members + m, share, 0.0), axis=1, keepdims=True)
            gate = jnp.dot(x, gate_ref[m], preferred_element_type=jnp.float32)
            up = jnp.dot(x, up_ref[m], preferred_element_type=jnp.float32)
            hidden_ref[at, m * units:(m + 1) * units] = (jax.nn.silu(gate) * up * scale).astype(hidden_ref.dtype)

    for d in range(1, nz + 3):
        if d < nz:
            pass_on(d)
        if d <= nz:
            pass_second(d - 1)
        if d == 3:
            for i in range(len(ep_rels)):
                w_sends[i].wait_send()
                ref = w_out_ref.at[0]
                pltpu.make_async_copy(ref, ref, w_recv.at[i]).wait()
            own.wait()
            w_own.wait()
            for load in loads:
                load.wait()
        if d >= 3:
            compute(d - 3)
        if 2 <= d <= nz + 1:
            pass_last(d - 2)
    for copy in sends:
        copy.wait_send()


def gather(sizes, x, w, gate, up):
    groups, parts = sizes[0] * sizes[1], sizes[2] * sizes[3]
    rows, cols = x.shape
    n_send = 2 * (sizes[0] - 1 + sizes[0] + 2 * sizes[0] + 4 * sizes[0])
    return pl.pallas_call(
        functools.partial(gather_kernel, sizes),
        out_shape=jax.ShapeDtypeStruct((groups * rows, gate.shape[0] * gate.shape[2]), x.dtype),
        in_specs=[pl.BlockSpec(memory_space=pltpu.VMEM)] * 2 + [pl.BlockSpec(memory_space=pl.ANY)] * 2,
        out_specs=pl.BlockSpec(memory_space=pltpu.VMEM),
        scratch_shapes=[
            pltpu.VMEM((groups * rows, parts * cols), x.dtype),
            pltpu.VMEM((groups,) + w.shape, w.dtype),
            pltpu.VMEM(gate.shape, gate.dtype),
            pltpu.VMEM(up.shape, up.dtype),
            pltpu.SemaphoreType.DMA((n_send,)),
            pltpu.SemaphoreType.DMA((2, groups * parts)),
            pltpu.SemaphoreType.DMA((groups - 1,)),
            pltpu.SemaphoreType.DMA((groups,)),
            pltpu.SemaphoreType.DMA,
            pltpu.SemaphoreType.DMA((2,)),
        ],
        compiler_params=pltpu.CompilerParams(collective_id=0, has_side_effects=True, vmem_limit_bytes=58 << 20),
        name="gather_hidden",
    )(x, w, gate, up)


def scatter_kernel(sizes, p_ref, out_ref, buf_c, buf_1, buf_2, buf_z, send_sem, recv_c, recv_1, recv_2, recv_z):
    nz = sizes[0]
    rows, cols = out_ref.shape
    half = rows // 2
    here = place(sizes)
    barrier(here, sizes, [(d, 0, 0, 0) for d in range(1, nz)] + [(0, 1, 0, 0), (0, 0, 1, 0), (0, 0, 0, 1)])
    axis = ((0, 1, 0, 0), (0, 0, 1, 0))
    first = {0: axis[1], 1: axis[0]}
    second = {0: axis[0], 1: axis[1]}
    sends = []

    def local(h, rel):
        group, member = device(moved(here, sizes, rel))
        return p_ref.at[pl.ds(pl.multiple_of(group * rows + h * half, half), half),
                        pl.ds(pl.multiple_of(member * cols, cols), cols)]

    def rel_of(h, a, b, d):
        e, f = (b, a) if h == 0 else (a, b)
        return (d, e, f)

    def send(src, dst, recv, step):
        copy = pltpu.make_async_remote_copy(
            src_ref=src, dst_ref=dst, send_sem=send_sem.at[len(sends)], recv_sem=recv,
            device_id=device(moved(here, sizes, step)), device_id_type=MESH)
        copy.start()
        sends.append(copy)

    def arrive(ref, sem):
        pltpu.make_async_copy(ref, ref, sem).wait()

    def add(dst, *srcs):
        chunk = 16

        @pl.loop(0, half // chunk)
        def _(i):
            at = pl.ds(pl.multiple_of(i * chunk, chunk), chunk)
            total = srcs[0][at, :].astype(jnp.float32)
            for src in srcs[1:]:
                total = total + src[at, :].astype(jnp.float32)
            dst[at, :] = total.astype(dst.dtype)

    zs = list(range(nz))[::-1]
    for d in zs:
        for a, b in ((1, 1), (1, 0), (0, 1), (0, 0)):
            for h in range(2):
                send(local(h, rel_of(h, a, b, d) + (1,)), buf_c.at[h, a, b, d], recv_c.at[h, a, b, d], (0, 0, 0, 1))

    def step_first(d):
        for b in (1, 0):
            for h in range(2):
                piece = buf_c.at[h, 1, b, d]
                arrive(piece, recv_c.at[h, 1, b, d])
                add(piece, piece, local(h, rel_of(h, 1, b, d) + (0,)))
                send(piece, buf_1.at[h, b, d], recv_1.at[h, b, d], first[h])

    def step_second(d):
        for h in range(2):
            piece = buf_c.at[h, 0, 1, d]
            arrive(piece, recv_c.at[h, 0, 1, d])
            arrive(buf_1.at[h, 1, d], recv_1.at[h, 1, d])
            add(piece, piece, local(h, rel_of(h, 0, 1, d) + (0,)), buf_1.at[h, 1, d])
            send(piece, buf_2.at[h, d], recv_2.at[h, d], second[h])

    def step_last(d):
        for h in range(2):
            piece = buf_c.at[h, 0, 0, d]
            arrive(piece, recv_c.at[h, 0, 0, d])
            arrive(buf_1.at[h, 0, d], recv_1.at[h, 0, d])
            arrive(buf_2.at[h, d], recv_2.at[h, d])
            srcs = (piece, local(h, rel_of(h, 0, 0, d) + (0,)), buf_1.at[h, 0, d], buf_2.at[h, d])
            if d:
                add(piece, *srcs)
                send(piece, buf_z.at[h, d - 1], recv_z.at[h, d - 1], (d, 0, 0, 0))
            else:
                for k in range(nz - 1):
                    arrive(buf_z.at[h, k], recv_z.at[h, k])
                add(out_ref.at[pl.ds(h * half, half), :], *srcs, *[buf_z.at[h, k] for k in range(nz - 1)])

    for i in range(nz + 2):
        if i < nz:
            step_first(zs[i])
        if 1 <= i <= nz:
            step_second(zs[i - 1])
        if i >= 2:
            step_last(zs[i - 2])
    for copy in sends:
        copy.wait_send()


def scatter(sizes, p):
    nz = sizes[0]
    groups, parts = nz * 2, sizes[2] * sizes[3]
    rows, cols = p.shape[0] // groups, p.shape[1] // parts
    half = rows // 2
    n_send = 2 * (4 * nz + 2 * nz + nz + nz - 1)
    return pl.pallas_call(
        functools.partial(scatter_kernel, sizes),
        out_shape=jax.ShapeDtypeStruct((rows, cols), p.dtype),
        in_specs=[pl.BlockSpec(memory_space=pltpu.VMEM)],
        out_specs=pl.BlockSpec(memory_space=pltpu.VMEM),
        scratch_shapes=[
            pltpu.VMEM((2, 2, 2, nz, half, cols), p.dtype),
            pltpu.VMEM((2, 2, nz, half, cols), p.dtype),
            pltpu.VMEM((2, nz, half, cols), p.dtype),
            pltpu.VMEM((2, nz - 1, half, cols), p.dtype),
            pltpu.SemaphoreType.DMA((n_send,)),
            pltpu.SemaphoreType.DMA((2, 2, 2, nz)),
            pltpu.SemaphoreType.DMA((2, 2, nz)),
            pltpu.SemaphoreType.DMA((2, nz)),
            pltpu.SemaphoreType.DMA((2, nz - 1)),
        ],
        compiler_params=pltpu.CompilerParams(collective_id=1, has_side_effects=True, vmem_limit_bytes=40 << 20),
        name="reduce_scatter",
    )(p)


def hidden_kernel(x_ref, w_ref, gate_ref, up_ref, out_ref):
    gate = jnp.dot(x_ref[...], gate_ref[0], preferred_element_type=jnp.float32)
    up = jnp.dot(x_ref[...], up_ref[0], preferred_element_type=jnp.float32)
    out_ref[...] = (jax.nn.silu(gate) * up * w_ref[0]).astype(out_ref.dtype)


def down_kernel(h_ref, down_ref, out_ref):
    out_ref[...] = jnp.dot(h_ref[...], down_ref[...], preferred_element_type=jnp.float32).astype(out_ref.dtype)


def tile_of(total, wanted):
    while total % wanted:
        wanted //= 2
    return wanted


def hidden_units(x, scale, gate_weight, up_weight):
    members, width, units = gate_weight.shape
    rows = x.shape[0]
    tile = tile_of(rows, 256)
    return pl.pallas_call(
        hidden_kernel,
        grid=(members, rows // tile),
        out_shape=jax.ShapeDtypeStruct((rows, members * units), x.dtype),
        in_specs=[
            pl.BlockSpec((tile, width), lambda e, m: (m, 0)),
            pl.BlockSpec((1, tile, 1), lambda e, m: (e, m, 0)),
            pl.BlockSpec((1, width, units), lambda e, m: (e, 0, 0)),
            pl.BlockSpec((1, width, units), lambda e, m: (e, 0, 0)),
        ],
        out_specs=pl.BlockSpec((tile, units), lambda e, m: (m, e)),
        compiler_params=pltpu.CompilerParams(vmem_limit_bytes=40 << 20),
        name="hidden",
    )(x, scale, gate_weight, up_weight)


def down_product(hidden, down_weight):
    members, units, width = down_weight.shape
    rows = hidden.shape[0]
    down = down_weight.reshape(members * units, width)
    tile_n = tile_of(width, 512)
    tile_m = tile_of(rows, 1024)
    return pl.pallas_call(
        down_kernel,
        grid=(rows // tile_m, width // tile_n),
        out_shape=jax.ShapeDtypeStruct((rows, width), hidden.dtype),
        in_specs=[
            pl.BlockSpec((tile_m, members * units), lambda m, n: (m, 0)),
            pl.BlockSpec((members * units, tile_n), lambda m, n: (0, n)),
        ],
        out_specs=pl.BlockSpec((tile_m, tile_n), lambda m, n: (m, n)),
        compiler_params=pltpu.CompilerParams(vmem_limit_bytes=50 << 20),
        name="down",
    )(hidden, down)


def body(tokens, expert_ids, gate_prob, gate_weight, up_weight, down_weight):
    groups, parts = lax.axis_size("ep"), lax.axis_size("etp")
    members = gate_weight.shape[0]
    numbers = jnp.arange(members * groups, dtype=jnp.int32)
    share = jnp.sum(jnp.where(expert_ids[:, :, None] == numbers, gate_prob[:, :, None], 0.0), axis=1)
    size = groups * parts * tokens.size * tokens.dtype.itemsize
    kernels = groups > 2 and groups & (groups - 1) == 0 and parts == 4 and size <= VMEM_BUDGET
    sizes = (groups // 2, 2, parts // 2, 2)
    if kernels:
        hidden = gather(sizes, tokens, share, gate_weight, up_weight)
        return scatter(sizes, down_product(hidden, down_weight))
    gathered = lax.all_gather(lax.all_gather(tokens, "ep", axis=0, tiled=True), "etp", axis=1, tiled=True)
    shares = lax.all_gather(share, "ep", axis=0, tiled=True)
    mine = lax.dynamic_slice_in_dim(shares, lax.axis_index("ep") * members, members, axis=1)
    hidden = hidden_units(gathered, jnp.transpose(mine)[:, :, None], gate_weight, up_weight)
    partial_sum = down_product(hidden, down_weight)
    summed = lax.psum_scatter(partial_sum, "etp", scatter_dimension=1, tiled=True)
    return lax.psum_scatter(summed, "ep", scatter_dimension=0, tiled=True)


def solution(mesh):
    in_specs = (
        P("ep", "etp"),
        P("ep", None),
        P("ep", None),
        P("ep", None, "etp"),
        P("ep", None, "etp"),
        P("ep", "etp", None),
    )
    out_specs = P("ep", "etp")
    return jax.shard_map(body, mesh=mesh, in_specs=in_specs, out_specs=out_specs, check_vma=False)
```
